32 devices in a mesh: row: 8 (over z, x), col: 4 (over y, core).
Axes of the slice: x: 2, y: 2, z: 4, core: 2. Of those that a mesh axis runs over, the one named last changes fastest.
Arguments:
- forward_map: float32 [2048, 16384], P('row', 'col'), may hold values from -0.125 to 0.125
- sensor_weights: float32 [2048], P('row'), may hold values from 0.25 to 4
- sensor_mask: int32 [2048], P('row'), may hold values 0 or 1
Outputs:
- gram_matrix: float32 [16384, 16384], P('row', 'col')
The draws below stay inside these ranges and needn't reach their ends.
All inputs are finite; a program needn't handle non-finite values. No bound on the sum of `sensor_mask` on one device may be relied on, other than what follows from the above.
Results may differ from the reference program's by a relative error of at most 0.000061.
Values sent between devices are 32-bit elements; how exact they have to be, the bound alone decides.
A program may use at most 128 MiB of HBM per device.

```python
import math
import jax
import jax.numpy as jnp
from jax import lax

PARAMS = 16384
OBS = 2048


def with_ends(array, stream_key, least, largest):
    longest = array.shape.index(max(array.shape))
    spots = []
    for shift in (0, 1):
        where = [jax.random.randint(jax.random.fold_in(stream_key, axis), (), 0, length) for axis, length in enumerate(array.shape)]
        where[longest] = (where[longest] + shift) % array.shape[longest]
        spots.append(tuple(where))
    return array.at[spots[0]].set(least).at[spots[1]].set(largest)


def level_of(own_key, extent, shards, least, largest):
    level, own = 1.0, jax.random.fold_in(own_key, 6)
    for dim, shards_of in shards:
        steps = jnp.exp(jax.random.uniform(jax.random.fold_in(own, dim), (shards_of,), jnp.float32, least / len(shards), largest / len(shards)))
        level = level * jnp.repeat(steps, extent[dim] // shards_of).reshape([-1 if axis == dim else 1 for axis in range(len(extent))])
    return level


def centred(own_key, shape, width, most, pieces=(), held_as=jnp.bfloat16):
    gain = level_of(own_key, shape, pieces, -0.22, 0.18) if pieces else 1.0
    result = jax.random.normal(own_key, shape, jnp.float32) * width * gain
    return jnp.minimum(jnp.maximum(result, -most), most).astype(held_as)


def setup_inputs(seed: int = 0) -> dict:
    key_of = jax.random.split(jax.random.key(seed), 4)
    return {
        "forward_map": centred(key_of[0], (OBS, PARAMS), OBS ** -0.5, 0.125, ((0, 8), (1, 4)), jnp.float32),
        "sensor_weights": jnp.clip(jnp.exp(math.log(4.0) - 2.7725887 * jax.random.uniform(key_of[1], (OBS,), jnp.float32) ** level_of(key_of[1], (OBS,), ((0, 8),), -0.2, 0.2)), 0.25, 4.0),
        "sensor_mask": with_ends((jax.random.randint(key_of[2], (OBS,), 0, 2) < 1).astype(jnp.int32), jax.random.fold_in(key_of[2], 1), 0, 1),
    }


def reference(forward_map, sensor_weights, sensor_mask):
    sensor_scale = sensor_weights * sensor_mask.astype(jnp.float32)
    weighted = forward_map * sensor_scale[:, None]
    return lax.dot_general(forward_map, weighted, (((0,), (0,)), ((), ())), precision=lax.Precision.HIGHEST, preferred_element_type=jnp.float32)
```

```python
import functools

import jax
import jax.numpy as jnp
from jax import lax
from jax.experimental import pallas as pl
from jax.experimental.pallas import tpu as pltpu
from jax.sharding import PartitionSpec as P

MESH = pl.DeviceIdType.MESH
PIECES = 2


def ring_place(row, rows_count):
    return jnp.where(row % 2 == 0, row // 2, rows_count - 1 - row // 2)


def ring_row(place, rows_count):
    half = (rows_count + 1) // 2
    return jnp.where(place < half, 2 * place, 2 * (rows_count - 1 - place) + 1)


def gather_kernel(own, ring, side, stage, side_stage, ring_send, ring_recv, side_send, side_recv, local_sem):
    rows_count = lax.axis_size("row")
    cols_count = lax.axis_size("col")
    _, _, height, columns = ring.shape
    side_columns = side.shape[3]
    row, col = lax.axis_index("row"), lax.axis_index("col")
    place = ring_place(row, rows_count)
    ahead = ring_row(lax.rem(place + 1, rows_count), rows_count)
    behind = ring_row(lax.rem(place + rows_count - 1, rows_count), rows_count)
    towards = (ahead, behind)
    first = row * side_columns // columns
    start = pl.multiple_of(lax.rem(row * side_columns, columns), 128)
    link = lax.rem(col - first + cols_count, cols_count)
    following = lax.rem(col + 1, cols_count)
    preceding = lax.rem(col + cols_count - 1, cols_count)

    barrier = pltpu.get_barrier_semaphore()
    for other in ((ahead, col), (behind, col), (row, following), (row, preceding)):
        pl.semaphore_signal(barrier, inc=1, device_id=other, device_id_type=MESH)
    pl.semaphore_wait(barrier, 4)

    width = columns // PIECES

    def ring_copy(way, step, piece):
        span = pl.ds(piece * width, width)
        source = own.at[way] if step == 0 else ring.at[way, step]
        return pltpu.make_async_remote_copy(
            src_ref=source.at[:, span],
            dst_ref=ring.at[way, step + 1, :, span],
            send_sem=ring_send.at[way, step, piece],
            recv_sem=ring_recv.at[way, step, piece],
            device_id=(towards[way], col),
            device_id_type=MESH,
        )

    def side_copy(way, step, from_ring):
        if from_ring:
            source = (own.at[way] if step == 0 else ring.at[way, step]).at[:, pl.ds(start, side_columns)]
        else:
            source = side.at[way, step]
        return pltpu.make_async_remote_copy(
            src_ref=source,
            dst_ref=side.at[way, step],
            send_sem=side_send.at[way, step],
            recv_sem=side_recv.at[way, step],
            device_id=(row, following),
            device_id_type=MESH,
        )

    def keep_in(way):
        return pltpu.make_async_copy(own.at[way], stage.at[way], local_sem.at[way])

    def keep_out(way):
        return pltpu.make_async_copy(stage.at[way], ring.at[way, 0], local_sem.at[way])

    def side_in(way, step):
        source = (own.at[way] if step == 0 else ring.at[way, step]).at[:, pl.ds(start, side_columns)]
        return pltpu.make_async_copy(source, side_stage.at[way], local_sem.at[2 + way])

    def side_out(way, step):
        return pltpu.make_async_copy(side_stage.at[way], side.at[way, step], local_sem.at[2 + way])

    for step in range(rows_count + 1):
        if step < rows_count:
            for piece in range(PIECES):
                for way in range(2):
                    if step > 0:
                        ring_copy(way, step - 1, piece).wait_recv()
                    if step < rows_count - 1:
                        ring_copy(way, step, piece).start()
        if step == 0:
            for way in range(2):
                keep_in(way).start()
            for way in range(2):
                keep_in(way).wait()
                keep_out(way).start()
        if step < rows_count:

            @pl.when(link == 0)
            def _():
                for way in range(2):
                    side_copy(way, step, True).start()
                for way in range(2):
                    if step > 0:
                        side_out(way, step - 1).wait()
                    side_in(way, step).start()
                for way in range(2):
                    side_in(way, step).wait()
                    side_out(way, step).start()

        if step > 0:

            @pl.when(link > 0)
            def _():
                for way in range(2):
                    side_copy(way, step - 1, False).wait_recv()

                    @pl.when(link < cols_count - 1)
                    def _():
                        side_copy(way, step - 1, False).start()

    for way in range(2):
        keep_out(way).wait()
        for step in range(rows_count - 1):
            for piece in range(PIECES):
                ring_copy(way, step, piece).wait_send()

    @pl.when(link == 0)
    def _():
        for way in range(2):
            side_out(way, rows_count - 1).wait()

    @pl.when(link < cols_count - 1)
    def _():
        for way in range(2):
            for step in range(rows_count):
                side_copy(way, step, False).wait_send()


def gather(own, rows_count, side_columns, call_id):
    _, height, columns = own.shape
    anywhere = pl.BlockSpec(memory_space=pl.ANY)
    return pl.pallas_call(
        gather_kernel,
        out_shape=(
            jax.ShapeDtypeStruct((2, rows_count, height, columns), jnp.float32),
            jax.ShapeDtypeStruct((2, rows_count, height, side_columns), jnp.float32),
        ),
        in_specs=[anywhere],
        out_specs=(anywhere, anywhere),
        scratch_shapes=[
            pltpu.VMEM((2, height, columns), jnp.float32),
            pltpu.VMEM((2, height, side_columns), jnp.float32),
            pltpu.SemaphoreType.DMA((2, rows_count, PIECES)),
            pltpu.SemaphoreType.DMA((2, rows_count, PIECES)),
            pltpu.SemaphoreType.DMA((2, rows_count)),
            pltpu.SemaphoreType.DMA((2, rows_count)),
            pltpu.SemaphoreType.DMA((4,)),
        ],
        compiler_params=pltpu.CompilerParams(collective_id=call_id, has_side_effects=True),
        name=f"gather{height}",
    )(own)


def split(value):
    high = value.astype(jnp.bfloat16)
    return high, (value - high.astype(jnp.float32)).astype(jnp.bfloat16)


def product_kernel(left, scale, right, out, left_parts, right_parts):
    depth, wide = left.shape
    block = min(128, wide)

    @pl.when(pl.program_id(1) == 0)
    def _():
        @pl.loop(0, wide // block)
        def _(index):
            span = pl.ds(pl.multiple_of(index * block, block), block)
            high, low = split((left[:, span] * scale[...]).T)
            left_parts[span, :depth] = high
            left_parts[span, depth : 2 * depth] = high
            left_parts[span, 2 * depth :] = low

    high, low = split(right[...])
    right_parts[:depth, :] = high
    right_parts[depth : 2 * depth, :] = low
    right_parts[2 * depth :, :] = high

    tall = min(256, wide)

    @pl.loop(0, wide // tall)
    def _(index):
        span = pl.ds(pl.multiple_of(index * tall, tall), tall)
        out[span, :] = jnp.dot(left_parts[span, :], right_parts[...], preferred_element_type=jnp.float32)


def product(left, scale, right):
    depth, tall = left.shape
    wide = right.shape[1]
    tile_tall, tile_wide = min(1024, tall), min(512, wide)
    return pl.pallas_call(
        product_kernel,
        grid=(tall // tile_tall, wide // tile_wide),
        out_shape=jax.ShapeDtypeStruct((tall, wide), jnp.float32),
        in_specs=[
            pl.BlockSpec((depth, tile_tall), lambda i, j: (0, i)),
            pl.BlockSpec((depth, 1), lambda i, j: (0, 0)),
            pl.BlockSpec((depth, tile_wide), lambda i, j: (0, j)),
        ],
        out_specs=pl.BlockSpec((tile_tall, tile_wide), lambda i, j: (i, j)),
        scratch_shapes=[
            pltpu.VMEM((tile_tall, 3 * depth), jnp.bfloat16),
            pltpu.VMEM((3 * depth, tile_wide), jnp.bfloat16),
        ],
        compiler_params=pltpu.CompilerParams(vmem_limit_bytes=60 * 1024 * 1024),
        name=f"product{depth}",
    )(left, scale, right)


def packed_path(capacity, call_id, operands):
    forward_map, scales = operands
    rows_count, local = scales.shape
    columns = forward_map.shape[1]
    row = lax.axis_index("row")
    chosen = scales != 0
    slots = jnp.where(chosen, jnp.cumsum(chosen.astype(jnp.int32), axis=1) - 1, -1)
    places = slots[:, None, :] == lax.broadcasted_iota(jnp.int32, (1, capacity, 1), 1)
    packed_scales = jnp.sum(jnp.where(places, scales[:, None, :], 0.0), axis=2)
    if capacity == local:
        own, packed_scales = forward_map, scales
    else:
        mine = lax.dynamic_index_in_dim(places, row, 0, keepdims=False)
        own = lax.dot(
            mine.astype(jnp.float32), forward_map, precision=lax.Precision.HIGHEST, preferred_element_type=jnp.float32
        )
    height = capacity // 2
    side_columns = columns * lax.axis_size("col") // rows_count
    ring, side = gather(own.reshape(2, height, columns), rows_count, side_columns, call_id)
    steps = jnp.arange(rows_count)
    place = ring_place(row, rows_count)
    order = [ring_row((place - steps) % rows_count, rows_count), ring_row((place + steps) % rows_count, rows_count)]
    scale = jnp.concatenate([packed_scales[order[0], :height], packed_scales[order[1], height:]]).reshape(-1, 1)
    depth = 2 * rows_count * height
    return product(side.reshape(depth, side_columns), scale, ring.reshape(depth, columns))


def per_device(forward_map, sensor_weights, sensor_mask):
    local = forward_map.shape[0]
    sensor_scale = sensor_weights * sensor_mask.astype(jnp.float32)
    scales = lax.all_gather(sensor_scale, "row", axis=0)
    most = jnp.max(jnp.sum((scales != 0).astype(jnp.int32), axis=1))
    capacities = sorted({-(-local * part // 256) * 16 for part in (9, 10)} | {local})
    branches = [functools.partial(packed_path, capacity, index) for index, capacity in enumerate(capacities)]
    level = sum((most > capacity).astype(jnp.int32) for capacity in capacities[:-1])
    return lax.switch(level, branches, (forward_map, scales))


def solution(mesh):
    placed = (P("row", "col"), P("row"), P("row"))
    return jax.shard_map(
        per_device, mesh=mesh, in_specs=placed, out_specs=P("row", "col"), check_vma=False
    )
```
